32 devices in a mesh: seq: 8 (over z, y), head: 4 (over x, core).
Axes of the slice: x: 2, y: 2, z: 4, core: 2. Of those that a mesh axis runs over, the one named last changes fastest.
Arguments:
- query_rows: bfloat16 [8192, 4096], P('seq', 'head'), may hold values from -6 to 6
- key_rows: bfloat16 [8192, 1024], P('seq', 'head'), may hold values from -6 to 6
- value_rows: bfloat16 [8192, 1024], P('seq', 'head'), may hold values from -6 to 6
- attn_out: bfloat16 [8192, 4096], P('seq', 'head'), may hold values from -4 to 4
- out_grad: bfloat16 [8192, 4096], P(('seq', 'head')), may hold values from -6 to 6
- block_index: int32 [64, 8], P('seq'), may hold values from 0 to 63, as said below
- block_count: int32 [64], P('seq'), may hold values from 1 to 8
Outputs:
- query_grad: bfloat16 [8192, 4096], P('seq', 'head')
- key_grad: bfloat16 [8192, 1024], P('seq', 'head')
- value_grad: bfloat16 [8192, 1024], P('seq', 'head')
The draws below stay inside these ranges and needn't reach their ends.
Inputs may be any that keep to these rules, and one draw needn't show every extreme that they name: `block_index`: row i lists distinct blocks, all at or before block i; its first entry is block i, and blocks i - 1, i - 2 and 0 are listed wherever they exist and differ from i. Entries at or past block_count[i] repeat block i. Counting with repetition the entries of the 8 query blocks of one index of seq that name blocks held by another index, leaving out block 0 and, for the index just below, its last two blocks: at most 4 for any pair of indices, and exactly 4 for some pair in every draw.
All inputs are finite; a program needn't handle non-finite values.
Results may differ from the reference program's by a relative error of at most 0.006.
Values may be sent and summed in bfloat16 or wider, within the bound.
A program may use at most 128 MiB of HBM per device.

```python
import jax
import jax.numpy as jnp
from jax import lax

HD = 128
HQ = 32
KVH = 8
BLK = 128
NF = 4
MAXB = 8
QB_DEV = 8
TOKENS = 8192
QBLOCKS = 64
CAP = 4
N_SEQ = 8


def draw_query_rows(key, part):
    values = jax.random.normal(jax.random.fold_in(key, 1), (TOKENS, HQ * HD), jnp.float32)
    return jnp.clip(values, -6.0, 6.0).astype(jnp.bfloat16)


def draw_key_rows(key, part):
    values = jax.random.normal(jax.random.fold_in(key, 3), (TOKENS, KVH * HD), jnp.float32)
    return jnp.clip(values, -6.0, 6.0).astype(jnp.bfloat16)


def layout_tables(key):
    base_key = jax.random.fold_in(key, 23)
    devices = jnp.arange(N_SEQ, dtype=jnp.int32)
    permutes = jax.vmap(lambda device: jax.random.permutation(jax.random.fold_in(base_key, device), QB_DEV * NF))(devices)
    shifts = jax.random.randint(jax.random.fold_in(base_key, 101), (N_SEQ, QB_DEV), 0, QB_DEV)
    kept_far = jax.random.randint(jax.random.fold_in(base_key, 102), (N_SEQ, QB_DEV, NF), 0, 4) > 0
    kept_far = kept_far | (devices == N_SEQ - 1)[:, None, None]
    row_ids = jnp.arange(QB_DEV, dtype=jnp.int32)
    slot_ids = jnp.arange(NF, dtype=jnp.int32)
    slot_order = row_ids[:, None] * NF + slot_ids[None, :]
    distance = 1 + permutes[:, slot_order] // CAP
    owner_dev = devices[:, None, None] - distance
    within = (shifts[:, :, None] + slot_ids[None, None, :]) % QB_DEV
    far_block = owner_dev * QB_DEV + within
    query_block = devices[:, None] * QB_DEV + row_ids[None, :]
    far_usable = kept_far & (owner_dev >= 0) & (far_block >= 1) & (far_block <= query_block[..., None] - 3)
    near = jnp.stack([query_block, query_block - 1, query_block - 2, jnp.zeros_like(query_block)], axis=-1)
    near_usable = jnp.stack([query_block >= 0, query_block >= 1, query_block >= 2, query_block >= 3], axis=-1)
    entries = jnp.concatenate([near, far_block], axis=-1)
    usable = jnp.concatenate([near_usable, far_usable], axis=-1)
    width = 4 + NF
    sorter = jnp.argsort((1 - usable.astype(jnp.int32)) * width + jnp.arange(width, dtype=jnp.int32), axis=-1)
    sorted_entries = jnp.take_along_axis(entries, sorter, axis=-1)
    sorted_usable = jnp.take_along_axis(usable, sorter, axis=-1)
    table = jnp.where(sorted_usable, sorted_entries, query_block[..., None]).astype(jnp.int32)
    counted = jnp.sum(usable.astype(jnp.int32), axis=-1)
    return (table.reshape(QBLOCKS, MAXB), counted.reshape(QBLOCKS))


def draw_block_index(key, part):
    return layout_tables(key)[0]


def draw_block_count(key, part):
    return layout_tables(key)[1]


def steps_of(rng, extent, pieces, low, top_value):
    def one(dim, shards_of):
        steps = jax.random.uniform(jax.random.fold_in(jax.random.fold_in(rng, 6), dim), (shards_of,), jnp.float32, low / len(pieces), top_value / len(pieces))
        return jnp.repeat(jnp.exp(steps), extent[dim] // shards_of).reshape((-1,) + (1,) * (len(extent) - dim - 1))

    factor_of = one(*pieces[0])
    for cut in pieces[1:]:
        factor_of = factor_of * one(*cut)
    return factor_of


def bell_draw(rng, shape, scale, reach, cuts=(), kind=jnp.bfloat16):
    level = steps_of(rng, shape, cuts, -0.22, 0.18) if cuts else 1.0
    values = jax.random.normal(rng, shape, jnp.float32) * scale * level
    return jnp.minimum(jnp.maximum(values, -reach), reach).astype(kind)


def setup_inputs(seed: int = 0) -> dict:
    key_of = jax.random.split(jax.random.key(seed), 8)
    query_rows = draw_query_rows(jax.random.fold_in(key_of[7], 71), 0)
    key_rows = draw_key_rows(jax.random.fold_in(key_of[7], 71), 0)
    value_rows = bell_draw(key_of[2], (TOKENS, KVH * HD), 1.0, 6.0, ((0, 8), (1, 4)))
    attn_out = bell_draw(key_of[3], (TOKENS, HQ * HD), 0.5, 4.0, ((0, 8), (1, 4)))
    out_grad = bell_draw(key_of[4], (TOKENS, HQ * HD), 1.0, 6.0, ((0, 32),))
    block_index = draw_block_index(jax.random.fold_in(key_of[7], 71), 0)
    block_count = draw_block_count(jax.random.fold_in(key_of[7], 71), 0)
    return dict(query_rows=query_rows, key_rows=key_rows, value_rows=value_rows, attn_out=attn_out, out_grad=out_grad, block_index=block_index, block_count=block_count)


def reference(query_rows, key_rows, value_rows, attn_out, out_grad, block_index, block_count):
    tokens = query_rows.shape[0]
    qblocks = tokens // BLK
    kv_heads = key_rows.shape[1] // HD
    group_size = query_rows.shape[1] // (kv_heads * HD)
    max_blocks = block_index.shape[1]
    scale_factor = HD ** -0.5
    query_blocks = query_rows.reshape(qblocks, BLK, kv_heads, group_size, HD)
    grad_blocks = out_grad.reshape(qblocks, BLK, kv_heads, group_size, HD)
    out_blocks = attn_out.reshape(qblocks, BLK, kv_heads, group_size, HD)
    key_blocks = key_rows.reshape(qblocks, BLK, kv_heads, HD)
    value_blocks = value_rows.reshape(qblocks, BLK, kv_heads, HD)
    offsets = jnp.arange(BLK, dtype=jnp.int32)

    def one_block(carry, inputs):
        key_acc, value_acc = carry
        row_number, query_tile, grad_tile, out_tile, tile_index, tile_count = inputs
        key_tile = key_blocks[tile_index].astype(jnp.float32)
        value_tile = value_blocks[tile_index].astype(jnp.float32)
        query_wide = query_tile.astype(jnp.float32)
        grad_wide = grad_tile.astype(jnp.float32)
        scores = jnp.einsum("rgqd,mcgd->gqrmc", query_wide, key_tile) * scale_factor
        query_pos = row_number * BLK + offsets
        key_pos = tile_index[:, None] * BLK + offsets[None, :]
        is_live = jnp.arange(max_blocks, dtype=jnp.int32)[:, None] < tile_count
        allowed = is_live[None] & (key_pos[None] <= query_pos[:, None, None])
        masked = jnp.where(allowed, scores, -jnp.inf)
        row_top = jnp.max(masked, axis=(3, 4), keepdims=True)
        exponent = jnp.exp(masked - row_top)
        probs_full = exponent / jnp.sum(exponent, axis=(3, 4), keepdims=True)
        probs_low = lax.optimization_barrier(probs_full.astype(jnp.bfloat16)).astype(jnp.float32)
        dprobs = jnp.einsum("rgqd,mcgd->gqrmc", grad_wide, value_tile)
        out_dot = jnp.sum(grad_wide * out_tile.astype(jnp.float32), axis=-1)
        out_dot = jnp.transpose(out_dot, (1, 2, 0))[..., None, None]
        dscores = lax.optimization_barrier((probs_full * (dprobs - out_dot)).astype(jnp.bfloat16)).astype(jnp.float32)
        query_grad_tile = jnp.einsum("gqrmc,mcgd->rgqd", dscores, key_tile) * scale_factor
        key_part = jnp.einsum("gqrmc,rgqd->mcgd", dscores, query_wide) * scale_factor
        value_part = jnp.einsum("gqrmc,rgqd->mcgd", probs_low, grad_wide)
        key_acc = key_acc.at[tile_index].add(key_part)
        value_acc = value_acc.at[tile_index].add(value_part)
        return (key_acc, value_acc), query_grad_tile.reshape(BLK, -1).astype(jnp.bfloat16)

    zeros_acc = jnp.zeros((qblocks, BLK, kv_heads, HD), jnp.float32)
    inputs = (jnp.arange(qblocks, dtype=jnp.int32), query_blocks, grad_blocks, out_blocks, block_index, block_count)
    (key_acc, value_acc), query_grad = lax.scan(one_block, (zeros_acc, zeros_acc), inputs)
    query_grad = query_grad.reshape(tokens, -1)
    key_grad = key_acc.reshape(tokens, -1).astype(jnp.bfloat16)
    value_grad = value_acc.reshape(tokens, -1).astype(jnp.bfloat16)
    return query_grad, key_grad, value_grad
```

```python
import functools

import jax
import jax.numpy as jnp
from jax import lax
from jax.experimental import pallas as pl
from jax.experimental.pallas import tpu as pltpu
from jax.sharding import PartitionSpec as P

HD = 128
GROUP = 4
BLK = 128
NF = 4
LOG2E = 1.4426950408889634


def shifted(value, axis, steps):
    count = lax.axis_size(axis)
    initial, last = (max(0, -steps), min(count, count - steps))
    return lax.ppermute(value, axis, [(source, source + steps) for source in range(initial, last)])


def spread_first(x, axis):
    count = lax.axis_size(axis)
    me = lax.axis_index(axis)
    step = 1
    while step < count:
        pairs = [(i, i + step) for i in range(step) if i + step < count]
        got = lax.ppermute(x, axis, pairs)
        x = jnp.where(me < step, x, got)
        step *= 2
    return x


def sum_to_first(x, axis):
    count = lax.axis_size(axis)
    step = 1
    while step < count:
        step *= 2
    step //= 2
    while step >= 1:
        pairs = [(i + step, i) for i in range(step) if i + step < count]
        x = x + lax.ppermute(x, axis, pairs)
        step //= 2
    return x


def live_far(block_index, block_count, device, qblocks):
    owner = block_index // qblocks
    within = block_index % qblocks
    max_blocks = block_index.shape[-1]
    live = jnp.arange(max_blocks, dtype=jnp.int32) < block_count[..., None]
    is_local = owner == device
    is_prev = (owner == device - 1) & (within >= qblocks - 2)
    is_first = (block_index == 0) & ~is_local & ~is_prev
    is_far = live & ~is_local & ~is_prev & ~is_first
    return owner, within, is_local, is_prev, is_first, is_far


def positions_of(block_index, block_count, device, qblocks, capacity):
    owner, within, is_local, is_prev, is_first, is_far = live_far(
        block_index, block_count, device, qblocks
    )
    flat_far = is_far.reshape(-1)
    flat_owner = owner.reshape(-1)
    order = jnp.arange(flat_far.shape[0], dtype=jnp.int32)
    earlier = (
        flat_far[None, :]
        & (flat_owner[None, :] == flat_owner[:, None])
        & (order[None, :] < order[:, None])
    )
    rank = jnp.sum(earlier.astype(jnp.int32), axis=1).reshape(block_index.shape)
    far_position = qblocks + 3 + owner * capacity + rank
    return jnp.where(
        is_local,
        within,
        jnp.where(is_prev, within + 2, jnp.where(is_first, qblocks + 2, far_position)),
    )


def asked_of(tables, counts, me, qblocks, capacity):
    devices = tables.shape[0]
    who = jnp.arange(devices, dtype=jnp.int32)[:, None, None]
    owner, within, _, _, _, is_far = live_far(tables, counts, who, qblocks)
    mine = (is_far & (owner == me)).reshape(devices, -1)
    order = jnp.arange(mine.shape[1], dtype=jnp.int32)
    earlier = mine[:, None, :] & (order[None, None, :] < order[None, :, None])
    rank = jnp.sum(earlier.astype(jnp.int32), axis=2)
    slots = jnp.arange(capacity, dtype=jnp.int32)
    chosen = mine[:, None, :] & (rank[:, None, :] == slots[None, :, None])
    blocks = jnp.where(chosen, within.reshape(devices, 1, -1), 0)
    return jnp.sum(blocks, axis=2).reshape(-1)


def serve_kernel(capacity, kv_heads, asked_ref, k_ref, v_ref, out_ref):
    base = pl.program_id(0) * capacity
    for c in range(capacity):
        start = pl.multiple_of(asked_ref[base + c] * BLK, BLK)
        for h in range(kv_heads):
            cols = slice(h * HD, (h + 1) * HD)
            rows = slice(c * BLK, (c + 1) * BLK)
            out_ref[rows, 2 * h * HD : (2 * h + 1) * HD] = k_ref[pl.ds(start, BLK), cols]
            out_ref[rows, (2 * h + 1) * HD : (2 * h + 2) * HD] = v_ref[pl.ds(start, BLK), cols]


def serve(asked, key_rows, value_rows, capacity):
    kv_heads = key_rows.shape[1] // HD
    width = 2 * kv_heads * HD
    devices = asked.shape[0] // capacity
    whole = pl.BlockSpec(key_rows.shape, lambda s, a: (0, 0))
    return pl.pallas_call(
        functools.partial(serve_kernel, capacity, kv_heads),
        grid_spec=pltpu.PrefetchScalarGridSpec(
            num_scalar_prefetch=1,
            grid=(devices,),
            in_specs=[whole, whole],
            out_specs=pl.BlockSpec((capacity * BLK, width), lambda s, a: (s, 0)),
        ),
        out_shape=jax.ShapeDtypeStruct((devices * capacity * BLK, width), key_rows.dtype),
        cost_estimate=pl.CostEstimate(flops=0, bytes_accessed=6 << 20, transcendentals=0),
        name="serve",
    )(asked, key_rows, value_rows)


def attend_kernel(
    qblocks, entries, pos_ref, cnt_ref, q_ref, g_ref, o_ref, k_ref, v_ref, near_ref, far_ref,
    dq_ref, own_ref, dnear_ref, dfar_ref, kv_ref, acc_ref,
):
    r = pl.program_id(1)
    near_top = qblocks + 3

    @pl.when(r == 0)
    def _():
        own_ref[...] = jnp.zeros_like(own_ref)
        dnear_ref[...] = jnp.zeros_like(dnear_ref)
        acc_ref[...] = jnp.zeros_like(acc_ref)

    def at(slot):
        return pl.ds(pl.multiple_of(slot * BLK, BLK), BLK)

    for e in range(entries):
        p = pos_ref[r * entries + e]
        rows = slice(e * BLK, (e + 1) * BLK)

        @pl.when(p < qblocks)
        def _():
            kv_ref[rows, :HD] = k_ref[at(p), :]
            kv_ref[rows, HD:] = v_ref[at(p), :]

        @pl.when((p >= qblocks) & (p < near_top))
        def _():
            kv_ref[rows, :] = near_ref[at(p - qblocks), :]

        @pl.when(p >= near_top)
        def _():
            kv_ref[rows, :] = far_ref[at(p - near_top), :]

    def stacked(ref):
        return jnp.concatenate([ref[:, g * HD : (g + 1) * HD] for g in range(GROUP)], axis=0)

    scale = HD ** (-0.5)
    q = stacked(q_ref)
    g = stacked(g_ref)
    keys = kv_ref[:, :HD]
    values = kv_ref[:, HD:]
    contract_last = (((1,), (1,)), ((), ()))
    scores = lax.dot_general(keys, q, contract_last, preferred_element_type=jnp.float32)
    count = cnt_ref[r]
    shape = (BLK, GROUP * BLK)
    causal = lax.broadcasted_iota(jnp.int32, shape, 0) <= (
        lax.broadcasted_iota(jnp.int32, shape, 1) % BLK
    )
    parts = [jnp.where(causal, scores[:BLK], -jnp.inf)]
    for e in range(1, entries):
        bias = jnp.where(e < count, 0.0, -jnp.inf).astype(jnp.float32)
        parts.append(scores[e * BLK : (e + 1) * BLK] + bias)
    masked = jnp.concatenate(parts, axis=0)
    top = jnp.max(masked, axis=0, keepdims=True)
    powers = jnp.exp2((masked - top) * (scale * LOG2E))
    total = jnp.sum(powers, axis=0, keepdims=True)
    probs = powers * (1.0 / total)
    probs_low = probs.astype(jnp.bfloat16)
    out_prod = g.astype(jnp.float32) * stacked(o_ref).astype(jnp.float32)
    out_dot = jnp.sum(jnp.transpose(out_prod), axis=0, keepdims=True)
    dprobs = lax.dot_general(values, g, contract_last, preferred_element_type=jnp.float32)
    dscores = (probs * (dprobs - out_dot)).astype(jnp.bfloat16)
    dq = jnp.dot(jnp.transpose(keys), dscores, preferred_element_type=jnp.float32) * scale
    dq = jnp.transpose(dq).astype(dq_ref.dtype)
    for i in range(GROUP):
        dq_ref[:, i * HD : (i + 1) * HD] = dq[i * BLK : (i + 1) * BLK]
    dkeys = jnp.dot(dscores, q, preferred_element_type=jnp.float32) * scale
    dvalues = jnp.dot(probs_low, g, preferred_element_type=jnp.float32)

    for e in range(entries):
        p = pos_ref[r * entries + e]
        dk = dkeys[e * BLK : (e + 1) * BLK]
        dv = dvalues[e * BLK : (e + 1) * BLK]

        def add(ref, slot, dk=dk, dv=dv):
            ref[at(slot), :HD] += dk
            ref[at(slot), HD:] += dv

        @pl.when(p < qblocks)
        def _():
            add(own_ref, p)

        @pl.when((p >= qblocks) & (p < near_top))
        def _():
            add(dnear_ref, p - qblocks)

        @pl.when(p >= near_top)
        def _():
            add(acc_ref, p - near_top)

    @pl.when(r == qblocks - 1)
    def _():
        dfar_ref[...] = acc_ref[...].astype(dfar_ref.dtype)


def attend(position, count, query_rows, grad_rows, attn_out, key_rows, value_rows, near, far):
    qblocks, entries = position.shape
    kv_heads = key_rows.shape[1] // HD
    rows = query_rows.shape[0]
    wide = GROUP * HD
    by_row = pl.BlockSpec((BLK, wide), lambda h, r, *_: (r, h))

    def by_head(height, width):
        return pl.BlockSpec((height, width), lambda h, r, *_: (0, h))

    f32 = jnp.float32
    pairs = qblocks * entries * kv_heads * GROUP
    return pl.pallas_call(
        functools.partial(attend_kernel, qblocks, entries),
        grid_spec=pltpu.PrefetchScalarGridSpec(
            num_scalar_prefetch=2,
            grid=(kv_heads, qblocks),
            in_specs=[
                by_row, by_row, by_row,
                by_head(rows, HD), by_head(rows, HD),
                by_head(near.shape[0], 2 * HD), by_head(far.shape[0], 2 * HD),
            ],
            out_specs=[
                by_row, by_head(rows, 2 * HD), by_head(near.shape[0], 2 * HD),
                by_head(far.shape[0], 2 * HD),
            ],
            scratch_shapes=[
                pltpu.VMEM((entries * BLK, 2 * HD), key_rows.dtype),
                pltpu.VMEM((far.shape[0], 2 * HD), f32),
            ],
        ),
        out_shape=[
            jax.ShapeDtypeStruct(query_rows.shape, query_rows.dtype),
            jax.ShapeDtypeStruct((rows, 2 * kv_heads * HD), f32),
            jax.ShapeDtypeStruct(near.shape, f32),
            jax.ShapeDtypeStruct(far.shape, far.dtype),
        ],
        compiler_params=pltpu.CompilerParams(
            dimension_semantics=("arbitrary", "arbitrary"), vmem_limit_bytes=56 << 20
        ),
        cost_estimate=pl.CostEstimate(
            flops=pairs * 10 * BLK * BLK * HD,
            bytes_accessed=24 << 20,
            transcendentals=pairs * BLK * BLK,
        ),
        name="attend",
    )(
        position.reshape(-1), count, query_rows, grad_rows, attn_out, key_rows, value_rows,
        near, far,
    )


def finish_kernel(qblocks, slots, asked_ref, own_ref, back_ref, prev_ref, first_ref,
                  dk_ref, dv_ref, acc_ref):
    acc_ref[...] = own_ref[...]
    acc_ref[:BLK] += first_ref[...]
    acc_ref[(qblocks - 2) * BLK :] += prev_ref[...].astype(jnp.float32)
    for s in range(slots):
        rows = pl.ds(pl.multiple_of(asked_ref[s] * BLK, BLK), BLK)
        acc_ref[rows, :] += back_ref[s * BLK : (s + 1) * BLK, :].astype(jnp.float32)
    dk_ref[...] = acc_ref[:, :HD].astype(dk_ref.dtype)
    dv_ref[...] = acc_ref[:, HD:].astype(dv_ref.dtype)


def finish(asked, own, back, prev, first, dtype):
    rows, width = own.shape
    kv_heads = width // (2 * HD)

    def by_head(height, columns):
        return pl.BlockSpec((height, columns), lambda h, a: (0, h))

    out = jax.ShapeDtypeStruct((rows, kv_heads * HD), dtype)
    return pl.pallas_call(
        functools.partial(finish_kernel, rows // BLK, asked.shape[0]),
        grid_spec=pltpu.PrefetchScalarGridSpec(
            num_scalar_prefetch=1,
            grid=(kv_heads,),
            in_specs=[by_head(x.shape[0], 2 * HD) for x in (own, back, prev, first)],
            out_specs=[by_head(rows, HD), by_head(rows, HD)],
            scratch_shapes=[pltpu.VMEM((rows, 2 * HD), jnp.float32)],
        ),
        out_shape=[out, out],
        cost_estimate=pl.CostEstimate(flops=0, bytes_accessed=8 << 20, transcendentals=0),
        name="finish",
    )(asked, own, back, prev, first)


def interleave(key_rows, value_rows):
    heads = key_rows.shape[1] // HD
    parts = []
    for h in range(heads):
        cols = slice(h * HD, (h + 1) * HD)
        parts += [key_rows[:, cols], value_rows[:, cols]]
    return jnp.concatenate(parts, axis=1)


def local(query_rows, key_rows, value_rows, attn_out, out_grad, block_index, block_count):
    seq_count = lax.axis_size("seq")
    me = lax.axis_index("seq")
    qblocks = query_rows.shape[0] // BLK
    capacity = qblocks * NF // seq_count
    width = 2 * key_rows.shape[1]
    tables = lax.all_gather(
        jnp.concatenate([block_index, block_count[:, None]], axis=1), "seq", axis=0
    )
    asked = asked_of(tables[..., :-1], tables[..., -1], me, qblocks, capacity)
    position = positions_of(block_index, block_count, me, qblocks, capacity)
    grad_rows = lax.all_to_all(out_grad, "head", split_axis=1, concat_axis=0, tiled=True)
    served = serve(asked, key_rows, value_rows, capacity)
    far = lax.all_to_all(served, "seq", split_axis=0, concat_axis=0, tiled=True)
    tail = interleave(key_rows[(qblocks - 2) * BLK :], value_rows[(qblocks - 2) * BLK :])
    head = interleave(key_rows[:BLK], value_rows[:BLK])
    near = jnp.concatenate([shifted(tail, "seq", 1), spread_first(head, "seq")], axis=0)
    query_grad, own, dnear, dfar = attend(
        position, block_count, query_rows, grad_rows, attn_out, key_rows, value_rows, near, far
    )
    back = lax.all_to_all(dfar, "seq", split_axis=0, concat_axis=0, tiled=True)
    prev = shifted(dnear[: 2 * BLK].astype(jnp.bfloat16), "seq", -1)
    mine = dnear[2 * BLK :]
    first = sum_to_first(mine, "seq")
    first = jnp.where(me == 0, first, jnp.zeros_like(first))
    key_grad, value_grad = finish(asked, own, back, prev, first, key_rows.dtype)
    return (query_grad, key_grad, value_grad)


def solution(mesh):
    return jax.shard_map(
        local,
        mesh=mesh,
        in_specs=(
            P("seq", "head"),
            P("seq", "head"),
            P("seq", "head"),
            P("seq", "head"),
            P(("seq", "head"), None),
            P("seq", None),
            P("seq"),
        ),
        out_specs=(P("seq", "head"), P("seq", "head"), P("seq", "head")),
        check_vma=False,
    )
```
